16 devices in a mesh: dp: 2 (over y, z), tp: 8 (over x, core).
Axes of the slice: x: 4, y: 2, z: 1, core: 2. Of those that a mesh axis runs over, the one named last changes fastest.
The devices are a block of a 4x4x8 slice.
Arguments:
- x: bfloat16 [4096, 12288], P('dp'), parts along dimension 0
- gain: bfloat16 [12288], replicated
- wq: bfloat16 [12288, 12288], P(None, 'tp')
- wk: bfloat16 [12288, 1024], P(None, 'tp')
- wv: bfloat16 [12288, 1024], P(None, 'tp')
- wo: bfloat16 [12288, 12288], P('tp')
Outputs:
- output: bfloat16 [4096, 12288], P('dp'), parts along dimension 0
There are 2 independent parts. The reference program is written for one: setup_inputs(seed, part) draws one part's arguments, and reference() takes and returns one part's arrays. A program takes and returns all parts, laid end to end along the dimension named above; an argument that names none is the same for every part.
All inputs are finite; a program needn't handle non-finite values.
Results may differ from the reference program's by a relative error of at most 0.012.
Values are sent between devices in bfloat16 or wider.
A program may use at most 768 MiB of HBM per device.

```python
import jax
import jax.numpy as jnp
from jax import lax

ROWS = 2048
D = 12288
HEADS = 96
KV_HEADS = 8
HEAD = 128
THETA = 10000


def setup_inputs(seed: int = 0, part: int = 0) -> dict:
    kx, kn, kq, kk, kv, ko = jax.random.split(jax.random.key(seed), 6)

    def weights(key, rows, columns):
        return jax.random.normal(key, (rows, columns), jnp.float32) * rows**-0.5

    drawn = {
        "x": jax.random.normal(jax.random.fold_in(kx, part), (ROWS, D), jnp.float32),
        "gain": 1 + 0.1 * jax.random.normal(kn, (D,), jnp.float32),
        "wq": 2 * weights(kq, D, HEADS * HEAD),
        "wk": 2 * weights(kk, D, KV_HEADS * HEAD),
        "wv": 4 * weights(kv, D, KV_HEADS * HEAD),
        "wo": weights(ko, HEADS * HEAD, D),
    }
    return {k: v.astype(jnp.bfloat16) for k, v in drawn.items()}


def normed(x, gain):
    wide = x.astype(jnp.float32)
    scale = lax.rsqrt(jnp.mean(wide * wide, -1, keepdims=True) + 1e-6)
    return (wide * scale * gain.astype(jnp.float32)).astype(jnp.bfloat16)


def turned(t, place, theta):
    half = t.shape[-1] // 2
    angle = place.astype(jnp.float32)[:, None] * theta ** (-jnp.arange(half, dtype=jnp.float32) / half)
    cos, sin = jnp.cos(angle)[:, None], jnp.sin(angle)[:, None]
    a, b = t[..., :half].astype(jnp.float32), t[..., half:].astype(jnp.float32)
    return jnp.concatenate([a * cos - b * sin, b * cos + a * sin], -1).astype(jnp.bfloat16)


def matmul(a, w):
    return jnp.dot(a, w, preferred_element_type=jnp.float32).astype(jnp.bfloat16)


def einsum(form, a, b):
    return jnp.einsum(form, a.astype(jnp.float32), b.astype(jnp.float32))


def attention(q, k, v):
    scores = einsum("tgsd,ugd->gstu", q, k) * q.shape[-1] ** -0.5
    token = jnp.arange(q.shape[0])
    scores = jnp.where(token[:, None] >= token, scores, -jnp.inf)
    weights = jax.nn.softmax(scores, -1).astype(jnp.bfloat16)
    return einsum("gstu,ugd->tgsd", weights, v).astype(jnp.bfloat16)


def reference(x, gain, wq, wk, wv, wo):
    a, place = normed(x, gain), jnp.arange(ROWS)
    q = turned(matmul(a, wq).reshape(ROWS, HEADS, HEAD), place, THETA).reshape(ROWS, KV_HEADS, -1, HEAD)
    k = turned(matmul(a, wk).reshape(ROWS, KV_HEADS, HEAD), place, THETA)
    v = matmul(a, wv).reshape(ROWS, KV_HEADS, HEAD)
    seen = attention(q, k, v).reshape(ROWS, HEADS * HEAD)
    return (x.astype(jnp.float32) + jnp.dot(seen, wo, preferred_element_type=jnp.float32)).astype(jnp.bfloat16)
```

```python
import functools

import jax
import jax.numpy as jnp
from jax import lax
from jax.experimental import pallas as pl
from jax.experimental.pallas import tpu as pltpu
from jax.sharding import PartitionSpec as P

HEAD = 128
THETA = 10000
NEG = -1e30
HIDDEN = 2 * NEG
LOG2E = 1.4426950408889634
VMEM = 66_900_000
BLOCK = 256
PAIR = 2
RING = 4
BUFFERS = 3
MESH = pl.DeviceIdType.MESH
F32, BF16 = jnp.float32, jnp.bfloat16


def _dot(a, b, ca=1, cb=0):
    return lax.dot_general(a, b, (((ca,), (cb,)), ((), ())), preferred_element_type=F32)


def _layer(axis, x_ref, gain_ref, cos_ref, sin_ref, wq_ref, wk_ref, wv_ref, wo_ref, y_ref, xa, wbuf, wkv, qacc, kvacc, q_s, k_s, vt_s, top_s,
           mix_s, seen_s, own_s, dsend, drecv, r1s, r1r, r2s, r2r, ys, xres, wsem, xsem, kvsem, ressem, ysem, d_ss, d_rs, d_free, r1_ss, r1_rs,
           r1_free, r2_ss, r2_rs, r2_free, a1_ss, a1_rs, a2_ss, a2_rs, p_ss, p_rs):
    rows, deep = x_ref.shape
    unit = r1s.shape[1]
    blocks = rows // BLOCK
    heads = unit // HEAD
    half = BLOCK // 2
    depth_tiles = deep // unit
    tiles = depth_tiles + 2 * RING
    me = lax.axis_index(axis)
    chip, core = me // 2, me % 2
    other = 1 - core
    right = ((chip + 1) % RING) * 2 + core
    left = ((chip + RING - 1) % RING) * 2 + core
    partner = chip * 2 + other
    upper, lower = pl.ds(0, half), pl.ds(half, half)

    barrier = pltpu.get_barrier_semaphore()
    for peer in (left, right, partner):
        pl.semaphore_signal(barrier, inc=1, device_id={axis: peer}, device_id_type=MESH)
    pl.semaphore_wait(barrier, 3)

    def remote(src, dst, ss, rs, peer):
        return pltpu.make_async_remote_copy(src_ref=src, dst_ref=dst, send_sem=ss, recv_sem=rs, device_id={axis: peer}, device_id_type=MESH)

    def signal(sem, peer):
        pl.semaphore_signal(sem, inc=1, device_id={axis: peer}, device_id_type=MESH)

    def columns(away, k):
        return pl.ds(pl.multiple_of(((chip + away) % RING) * (2 * unit) + k * unit, unit), unit)

    def yref(b, part, away):
        start, size = part
        return y_ref.at[pl.ds(pl.multiple_of(b * BLOCK + start, half), size), columns(away, core)]

    whole, up, low = (0, BLOCK), (0, half), (half, half)

    def start_tile(g):
        i, slot = g % tiles, g % BUFFERS

        @pl.when(g < blocks * tiles)
        def _():
            @pl.when(i < depth_tiles)
            def _():
                at = pl.ds(pl.multiple_of(i * unit, unit), unit)
                pltpu.make_async_copy(wq_ref.at[at, :], wbuf.at[slot], wsem.at[slot]).start()

            @pl.when(i >= depth_tiles)
            def _():
                j = i - depth_tiles
                k = (other + j // RING) % 2
                away = (2 + RING - j % RING) % RING
                pltpu.make_async_copy(wo_ref.at[:, columns(away, k)], wbuf.at[slot], wsem.at[slot]).start()

    def wait_tile(g):
        slot = g % BUFFERS
        pltpu.make_async_copy(wq_ref.at[pl.ds(0, unit), :], wbuf.at[slot], wsem.at[slot]).wait()
        return slot

    def x_copy(b):
        return pltpu.make_async_copy(x_ref.at[pl.ds(pl.multiple_of(b * BLOCK, BLOCK), BLOCK), :], xa, xsem)

    kv_copies = [pltpu.make_async_copy(w, wkv.at[:, pl.ds(n * HEAD, HEAD)], kvsem.at[n]) for n, w in enumerate((wk_ref, wv_ref))]

    def d_copy(j):
        return remote(dsend.at[j], drecv.at[j], d_ss.at[j], d_rs.at[j], partner)

    r1_copies = [remote(r1s.at[upper], r1r.at[upper], r1_ss.at[0], r1_rs.at[0], left),
                 remote(r1s.at[lower], r1r.at[lower], r1_ss.at[1], r1_rs.at[1], right)]
    r2_copies = [remote(r2s.at[0], r2r.at[0], r2_ss.at[0], r2_rs.at[0], left), remote(r2s.at[1], r2r.at[1], r2_ss.at[1], r2_rs.at[1], right)]

    def a1_copies(b):
        p = b % 2
        mine = yref(b, whole, 0)
        return [remote(ys, mine, a1_ss.at[0], a1_rs.at[p, 0], left), remote(ys, mine, a1_ss.at[1], a1_rs.at[p, 1], right),
                remote(ys, mine, a1_ss.at[2], p_rs, partner)]

    def a1_arrived(b):
        p = b % 2
        for n in range(2):
            remote(ys, yref(b, whole, 0), a1_ss.at[n], a1_rs.at[p, n], left).wait_recv()

    def a2_copies(b):
        p = b % 2
        return [remote(yref(b, low, 1), yref(b, low, 1), a2_ss.at[0], a2_rs.at[p, 0], left),
                remote(yref(b, up, RING - 1), yref(b, up, RING - 1), a2_ss.at[1], a2_rs.at[p, 1], right)]

    def p_copy(b, n):
        away = (1, RING - 1, 2)[n]
        return remote(yref(b, whole, away), yref(b, whole, away), p_ss.at[n], p_rs, partner)

    def y_copy(b):
        return pltpu.make_async_copy(ys, yref(b, whole, 0), ysem)

    def res_copy(b):
        return pltpu.make_async_copy(x_ref.at[pl.ds(pl.multiple_of(b * BLOCK, BLOCK), BLOCK), columns(0, core)], xres, ressem)

    def passes(body, step=32):
        def one(r, _):
            body(pl.ds(pl.multiple_of(r * step, step), step))
        lax.fori_loop(0, BLOCK // step, one, None)

    def fourth_arrived(b):
        for c in a2_copies(b):
            c.wait_recv()

        @pl.when(b > 0)
        def _():
            p_copy(b, 2).wait_send()
        p_copy(b, 2).start()

    def fourth(b):
        a1_arrived(b)

        @pl.when(b > 0)
        def _():
            for c in (*a2_copies(b), p_copy(b, 0), p_copy(b, 1)):
                c.wait_send()
        for c in (*a2_copies(b), p_copy(b, 0), p_copy(b, 1)):
            c.start()

    def third(b):
        res_copy(b).start()
        for c in r2_copies:
            c.wait_recv()

        @pl.when(b > 0)
        def _():
            for c in a1_copies(b):
                c.wait_send()
            y_copy(b).wait()
        res_copy(b).wait()

        def finish(at):
            total = own_s[2 + b % 2, at, :] + r2r[0, at, :].astype(F32) + r2r[1, at, :].astype(F32)
            ys[at, :] = (xres[at, :].astype(F32) + total).astype(BF16)
        passes(finish)

        @pl.when(b < blocks - 1)
        def _():
            signal(r2_free.at[0], right)
            signal(r2_free.at[1], left)
        for c in a1_copies(b):
            c.start()
        y_copy(b).start()

    def second(b):
        for c in r1_copies:
            c.wait_recv()

        @pl.when(b > 0)
        def _():
            for c in r2_copies:
                c.wait_send()

        def add(at, r):
            came = r1r[at, :].astype(F32)
            first = r < half // 32
            r2s[0, at, :] = (own_s[1, at, :] + jnp.where(first, came, 0.0)).astype(BF16)
            r2s[1, at, :] = (own_s[0, at, :] + jnp.where(first, 0.0, came)).astype(BF16)

        def one(r, _):
            add(pl.ds(pl.multiple_of(r * 32, 32), 32), r)
        lax.fori_loop(0, BLOCK // 32, one, None)

        @pl.when(b < blocks - 1)
        def _():
            signal(r1_free.at[0], right)
            signal(r1_free.at[1], left)

        @pl.when(b > 0)
        def _():
            for n in range(2):
                pl.semaphore_wait(r2_free.at[n], 1)
        for c in r2_copies:
            c.start()

    def attend(b):
        e = HEAD**-0.5 * LOG2E
        wide = PAIR * BLOCK
        for n in range(heads // PAIR):
            top_s[n] = jnp.full((1, wide), NEG, F32)
            mix_s[n] = jnp.zeros(mix_s.shape[1:], F32)

        def block(j, masked):
            keys = k_s[j]
            values = vt_s[j]
            if masked:
                ok = lax.rem(lax.broadcasted_iota(jnp.int32, (BLOCK, wide), 1), BLOCK) >= lax.broadcasted_iota(jnp.int32, (BLOCK, wide), 0)
            per = 3
            for base in range(0, heads // PAIR, per):
                strips = range(base, min(base + per, heads // PAIR))
                scores = [_dot(keys, q_s[n], 1, 1) for n in strips]
                weights, keeps = [], []
                for n, s in zip(strips, scores):
                    if masked:
                        s = jnp.where(ok, s, HIDDEN)
                    old = top_s[n]
                    top = jnp.maximum(old, s.max(axis=0, keepdims=True))
                    top_s[n] = top
                    weights.append(jnp.exp2((s - top) * e).astype(BF16))
                    keeps.append(jnp.exp2((old - top) * e))
                for n, p, keep in zip(strips, weights, keeps):
                    mix_s[n] = mix_s[n] * keep + _dot(values, p)

        lax.fori_loop(0, b, lambda j, _: block(j, False), None)
        block(b, True)
        for n in range(heads // PAIR):
            out = mix_s[n, :HEAD, :] * (1 / mix_s[n, HEAD : HEAD + 1, :])
            for i in range(PAIR):
                at = (n * PAIR + i) * HEAD
                seen_s[:, at : at + HEAD] = out[:, i * BLOCK : (i + 1) * BLOCK].T.astype(BF16)

    def compute(b):
        first_tile = b * tiles
        x_copy(b).wait()

        def norm(at):
            total = jnp.zeros((at.size, 1), F32)
            for n in range(0, deep, unit):
                part = xa[at, n : n + unit].astype(F32)
                total += jnp.sum(part * part, axis=1, keepdims=True)
            scale = lax.rsqrt(total / deep + 1e-6)
            for n in range(0, deep, unit):
                part = xa[at, n : n + unit].astype(F32)
                xa[at, n : n + unit] = (part * scale * gain_ref[:, n : n + unit].astype(F32)).astype(BF16)
        passes(norm, 16)

        qacc[...] = jnp.zeros(qacc.shape, F32)
        kvacc[...] = jnp.zeros(kvacc.shape, F32)

        @pl.when(b == 0)
        def _():
            for c in kv_copies:
                c.wait()

        def project(i, _):
            g = first_tile + i
            start_tile(g + 2)
            slot = wait_tile(g)
            at = pl.ds(pl.multiple_of(i * unit, unit), unit)
            a = xa[:, at]
            for n in range(0, unit, 512):
                qacc[:, n : n + 512] += _dot(a, wbuf[slot, :, n : n + 512])
            kvacc[...] += _dot(a, wkv[at, :])
        lax.fori_loop(0, depth_tiles, project, None)

        @pl.when(b < blocks - 1)
        def _():
            x_copy(b + 1).start()

        at = pl.ds(pl.multiple_of(b * BLOCK, BLOCK), BLOCK)
        cos, sin = cos_ref[at, :], sin_ref[at, :]

        def turned(t):
            t = t.astype(BF16).astype(F32)
            return (t * cos + pltpu.roll(t, HEAD // 2, 1) * sin).astype(BF16)
        for n in range(heads):
            i = n % PAIR
            q_s[n // PAIR, i * BLOCK : (i + 1) * BLOCK, :] = turned(qacc[:, n * HEAD : (n + 1) * HEAD])
        k_s[b] = turned(kvacc[:, :HEAD])
        vt_s[b, :HEAD, :] = kvacc[:, HEAD:].T.astype(BF16)
        vt_s[b, HEAD:, :] = jnp.ones((vt_s.shape[1] - HEAD, BLOCK), BF16)
        attend(b)

        def give(j, _):
            g = first_tile + depth_tiles + j
            start_tile(g + 2)
            slot = wait_tile(g)

            @pl.when(b > 0)
            def _():
                d_copy(j).wait_send()
            for n in range(0, unit, 512):
                dsend[j, :, n : n + 512] = _dot(seen_s[...], wbuf[slot, :, n : n + 512]).astype(BF16)

            @pl.when(b > 0)
            def _():
                pl.semaphore_wait(d_free.at[j], 1)
            d_copy(j).start()
        lax.fori_loop(0, RING, give, None)

        for j in range(RING):
            g = first_tile + depth_tiles + RING + j
            start_tile(g + 2)
            slot = wait_tile(g)
            d_copy(j).wait_recv()
            if j == 0:
                @pl.when(b > 0)
                def _():
                    for c in r1_copies:
                        c.wait_send()
            for n in range(0, unit, 512):
                value = _dot(seen_s[...], wbuf[slot, :, n : n + 512]) + drecv[j, :, n : n + 512].astype(F32)
                if j == 0:
                    r1s[:, n : n + 512] = value.astype(BF16)
                else:
                    own_s[(0, 2 + b % 2, 1)[j - 1], :, n : n + 512] = value

            @pl.when(b < blocks - 1)
            def _():
                signal(d_free.at[j], partner)
            if j == 0:
                @pl.when(b > 0)
                def _():
                    for n in range(2):
                        pl.semaphore_wait(r1_free.at[n], 1)
                for c in r1_copies:
                    c.start()

    x_copy(0).start()
    start_tile(0)
    start_tile(1)
    for c in kv_copies:
        c.start()

    def step(t, _):
        for back, stage in ((4, fourth_arrived), (3, fourth), (2, third), (1, second)):
            b = t - back

            @pl.when((b >= 0) & (b < blocks))
            def _():
                stage(b)

        @pl.when(t < blocks)
        def _():
            compute(t)
    lax.fori_loop(0, blocks + 4, step, None)

    last = blocks - 1
    for j in range(RING):
        d_copy(j).wait_send()
    for c in (*r1_copies, *r2_copies, *a1_copies(last), *a2_copies(last), *(p_copy(last, n) for n in range(3))):
        c.wait_send()
    y_copy(last).wait()
    theirs = y_ref.at[:, pl.ds(0, RING * unit)]
    pltpu.make_async_copy(theirs, theirs, p_rs).wait()


def solution(mesh):
    axis = mesh.axis_names[1]
    group = mesh.shape[axis]

    def step(x, gain, wq, wk, wv, wo):
        rows, deep = x.shape
        unit = deep // group
        blocks = rows // BLOCK
        heads = unit // HEAD
        part = HEAD // 2
        angle = jnp.arange(rows).astype(F32)[:, None] * THETA ** (-jnp.arange(part, dtype=F32) / part)
        cos, sin = jnp.cos(angle), jnp.sin(angle)
        cos, sin = jnp.concatenate([cos, cos], 1), jnp.concatenate([-sin, sin], 1)
        vmem, hbm = pl.BlockSpec(memory_space=pltpu.VMEM), pl.BlockSpec(memory_space=pl.ANY)
        dma, regular = pltpu.SemaphoreType.DMA, pltpu.SemaphoreType.REGULAR
        strips = heads // PAIR
        return pl.pallas_call(
            functools.partial(_layer, axis),
            out_shape=jax.ShapeDtypeStruct((rows, deep), BF16),
            in_specs=[hbm, vmem, vmem, vmem, hbm, hbm, hbm, hbm],
            out_specs=hbm,
            scratch_shapes=[
                pltpu.VMEM((BLOCK, deep), BF16),
                pltpu.VMEM((BUFFERS, unit, unit), BF16),
                pltpu.VMEM((deep, 2 * HEAD), BF16),
                pltpu.VMEM((BLOCK, unit), F32),
                pltpu.VMEM((BLOCK, 2 * HEAD), F32),
                pltpu.VMEM((strips, PAIR * BLOCK, HEAD), BF16),
                pltpu.VMEM((blocks, BLOCK, HEAD), BF16),
                pltpu.VMEM((blocks, HEAD + 16, BLOCK), BF16),
                pltpu.VMEM((strips, 1, PAIR * BLOCK), F32),
                pltpu.VMEM((strips, HEAD + 16, PAIR * BLOCK), F32),
                pltpu.VMEM((BLOCK, unit), BF16),
                pltpu.VMEM((4, BLOCK, unit), F32),
                pltpu.VMEM((RING, BLOCK, unit), BF16),
                pltpu.VMEM((RING, BLOCK, unit), BF16),
                pltpu.VMEM((BLOCK, unit), BF16),
                pltpu.VMEM((BLOCK, unit), BF16),
                pltpu.VMEM((2, BLOCK, unit), BF16),
                pltpu.VMEM((2, BLOCK, unit), BF16),
                pltpu.VMEM((BLOCK, unit), BF16),
                pltpu.VMEM((BLOCK, unit), BF16),
                dma((BUFFERS,)), dma, dma((2,)), dma, dma,
                dma((RING,)), dma((RING,)), regular((RING,)),
                dma((2,)), dma((2,)), regular((2,)),
                dma((2,)), dma((2,)), regular((2,)),
                dma((3,)), dma((2, 2)),
                dma((2,)), dma((2, 2)),
                dma((3,)), dma,
            ],
            compiler_params=pltpu.CompilerParams(collective_id=0, has_side_effects=True, vmem_limit_bytes=VMEM),
        )(x, gain[None], cos, sin, wq, wk, wv, wo)

    tokens, columns = P(mesh.axis_names[0], None), P(None, axis)
    return jax.shard_map(
        step,
        mesh=mesh,
        in_specs=(tokens, P(None), columns, columns, columns, P(axis, None)),
        out_specs=tokens,
        check_vma=False,
    )
```

```python
import functools

import jax
import jax.numpy as jnp
import numpy as np
from jax import lax
from jax.experimental import pallas as pl
from jax.experimental.pallas import tpu as pltpu
from jax.sharding import PartitionSpec as P

HEAD = 128
THETA = 10000
NEG = -1e30
HIDDEN = 2 * NEG
LOG2E = 1.4426950408889634
VMEM = 66_900_000
BLOCK = 256
PAIR = 2
RING = 4
BUFFERS = 3
FIRST = 9
WORK = 2_000_000_000
COPIES = 8
PARTS = 4
AWAY = (2, 1, RING - 1, 0)
ORDER = ((True, 0), (True, 1), (False, 0), (True, 2), (False, 1), (True, 3), (False, 2), (False, 3))
MESH = pl.DeviceIdType.MESH
F32, BF16 = jnp.float32, jnp.bfloat16


def _dot(a, b, ca=1, cb=0):
    return lax.dot_general(a, b, (((ca,), (cb,)), ((), ())), preferred_element_type=F32)


def _layer(axis, x_ref, gain_ref, table_ref, wq_ref, wk_ref, wv_ref, wo_ref, y_ref, last_ref, xa, table, gains, wbuf, wkv, qacc, kvacc, q_s, k_s, vt_s, top_s,
           mix_s, seen_s, own_s, dsend, drecv, r1s, r1r, r2s, r2r, ys, xres, wsem, xsem, tsem, gsem, kvsem, ressem, ysem, d_ss, d_rs, d_free, r1_ss, r1_rs,
           r1_free, r2_ss, r2_rs, r2_free, a1_ss, a1_rs, a2_ss, a2_rs, p_ss, p_rs):
    rows, deep = x_ref.shape
    unit = r1s.shape[1]
    blocks = rows // BLOCK
    last = blocks - 1
    heads = unit // HEAD
    half = BLOCK // 2
    depth_tiles = deep // unit
    tiles = depth_tiles + 2 * RING
    me = lax.axis_index(axis)
    chip, core = me // 2, me % 2
    other = 1 - core
    right = ((chip + 1) % RING) * 2 + core
    left = ((chip + RING - 1) % RING) * 2 + core
    partner = chip * 2 + other
    upper, lower = pl.ds(0, half), pl.ds(half, half)

    def remote(src, dst, ss, rs, peer):
        return pltpu.make_async_remote_copy(src_ref=src, dst_ref=dst, send_sem=ss, recv_sem=rs, device_id={axis: peer}, device_id_type=MESH)

    def signal(sem, peer):
        pl.semaphore_signal(sem, inc=1, device_id={axis: peer}, device_id_type=MESH)

    def columns(away, k):
        return pl.ds(pl.multiple_of(((chip + away) % RING) * (2 * unit) + k * unit, unit), unit)

    def yref(b, part, away):
        start, size = part
        return y_ref.at[pl.ds(pl.multiple_of(b * BLOCK + start, half // 2), size), columns(away, core)]

    whole = (0, BLOCK)

    def start_wq(b, i):
        slot = (b * tiles + i) % BUFFERS
        at = pl.ds(pl.multiple_of(i * unit, unit), unit)
        pltpu.make_async_copy(wq_ref.at[at, :], wbuf.at[slot], wsem.at[slot]).start()

    def start_wo(b, i):
        slot = (b * tiles + depth_tiles + i) % BUFFERS
        give, j = ORDER[i]
        pltpu.make_async_copy(wo_ref.at[:, columns(AWAY[j], other if give else core)], wbuf.at[slot], wsem.at[slot]).start()

    def wait_tile(g):
        slot = g % BUFFERS
        pltpu.make_async_copy(wq_ref.at[pl.ds(0, unit), :], wbuf.at[slot], wsem.at[slot]).wait()
        return slot

    def x_copies(b):
        made = []
        for n in range(PARTS):
            size = BLOCK // PARTS
            made.append(pltpu.make_async_copy(x_ref.at[pl.ds(pl.multiple_of(b * BLOCK + n * size, size), size), :], xa.at[pl.ds(n * size, size), :],
                                              xsem.at[n]))
        return made

    table_copy = pltpu.make_async_copy(table_ref, table, tsem)
    gain_copy = pltpu.make_async_copy(gain_ref, gains, gsem)
    kv_copies = [pltpu.make_async_copy(w, wkv.at[:, pl.ds(n * HEAD, HEAD)], kvsem.at[n]) for n, w in enumerate((wk_ref, wv_ref))]

    def d_copy(j):
        return remote(dsend.at[j], drecv.at[j], d_ss.at[j], d_rs.at[j], partner)

    r1_copies = [remote(r1s.at[upper], r1r.at[upper], r1_ss.at[0], r1_rs.at[0], left),
                 remote(r1s.at[lower], r1r.at[lower], r1_ss.at[1], r1_rs.at[1], right)]
    r2_copies = [remote(r2s.at[0], r2r.at[0], r2_ss.at[0], r2_rs.at[0], left), remote(r2s.at[1], r2r.at[1], r2_ss.at[1], r2_rs.at[1], right)]

    def a1_copies(b):
        p = b % 2
        mine = yref(b, whole, 0)
        return [remote(ys, mine, a1_ss.at[0], a1_rs.at[p, 0], left), remote(ys, mine, a1_ss.at[1], a1_rs.at[p, 1], right),
                remote(ys, mine, a1_ss.at[2], p_rs, partner)]

    def a1_arrived(b):
        p = b % 2
        for n in range(2):
            remote(ys, yref(b, whole, 0), a1_ss.at[n], a1_rs.at[p, n], left).wait_recv()

    def a2_copies(b, parts=(0, 1)):
        p, made = b % 2, []
        for n in parts:
            for to, away, start, peer in ((0, 1, half, left), (1, RING - 1, 0, right)):
                piece = yref(b, (start + n * (half // 2), half // 2), away)
                made.append(remote(piece, piece, a2_ss.at[2 * n + to], a2_rs.at[p, 2 * n + to], peer))
        return made

    def p_copy(b, n):
        away = (1, RING - 1, 2)[n]
        return remote(yref(b, whole, away), yref(b, whole, away), p_ss.at[n], p_rs, partner)

    def y_copy(b):
        return pltpu.make_async_copy(ys, yref(b, whole, 0), ysem)

    def res_copy(b):
        return pltpu.make_async_copy(x_ref.at[pl.ds(pl.multiple_of(b * BLOCK, BLOCK), BLOCK), columns(0, core)], xres, ressem)

    def passes(body, step=32, start=0, size=BLOCK):
        def one(r, _):
            body(pl.ds(pl.multiple_of(start + r * step, step), step))
        lax.fori_loop(0, size // step, one, None)

    def fourth_arrived(b):
        for c in a2_copies(b):
            c.wait_recv()

        @pl.when(b > 0)
        def _():
            p_copy(b, 2).wait_send()
        p_copy(b, 2).start()

    def fourth(b):
        a1_arrived(b)

        @pl.when(b > 0)
        def _():
            for c in (*a2_copies(b), p_copy(b, 0), p_copy(b, 1)):
                c.wait_send()
        for c in (*a2_copies(b, (0,)), p_copy(b, 0), p_copy(b, 1)):
            c.start()

    def fourth_rest(b):
        for c in a2_copies(b, (1,)):
            c.start()

    def third(b):
        res_copy(b).start()
        for c in r2_copies:
            c.wait_recv()

        @pl.when(b > 0)
        def _():
            for c in a1_copies(b):
                c.wait_send()
            y_copy(b).wait()
        res_copy(b).wait()

        def finish(at):
            total = own_s[2, at, :] + r2r[0, at, :].astype(F32) + r2r[1, at, :].astype(F32)
            ys[at, :] = (xres[at, :].astype(F32) + total).astype(BF16)
        passes(finish)

        @pl.when(b < blocks - 1)
        def _():
            signal(r2_free.at[0], right)
            signal(r2_free.at[1], left)

        @pl.when(b < last)
        def _():
            for c in a1_copies(b):
                c.start()
            y_copy(b).start()

        @pl.when(b == last)
        def _():
            pltpu.make_async_copy(ys, last_ref, ysem).start()

    def second(b):
        for c in r1_copies:
            c.wait_recv()

        @pl.when(b > 0)
        def _():
            for c in r2_copies:
                c.wait_send()

        def add(at, r):
            came = r1r[at, :].astype(F32)
            first = r < half // 32
            r2s[0, at, :] = (own_s[1, at, :] + jnp.where(first, came, 0.0)).astype(BF16)
            r2s[1, at, :] = (own_s[0, at, :] + jnp.where(first, 0.0, came)).astype(BF16)

        def one(r, _):
            add(pl.ds(pl.multiple_of(r * 32, 32), 32), r)
        lax.fori_loop(0, BLOCK // 32, one, None)

        @pl.when(b < blocks - 1)
        def _():
            signal(r1_free.at[0], right)
            signal(r1_free.at[1], left)

        @pl.when(b > 0)
        def _():
            for n in range(2):
                pl.semaphore_wait(r2_free.at[n], 1)
        for c in r2_copies:
            c.start()

    def attend(b):
        e = HEAD**-0.5 * LOG2E
        wide = PAIR * BLOCK
        for n in range(heads // PAIR):
            top_s[n] = jnp.full((1, wide), NEG, F32)
            mix_s[n] = jnp.zeros(mix_s.shape[1:], F32)

        def block(j, masked):
            keys = k_s[j]
            values = vt_s[j]
            if masked:
                ok = lax.rem(lax.broadcasted_iota(jnp.int32, (BLOCK, wide), 1), BLOCK) >= lax.broadcasted_iota(jnp.int32, (BLOCK, wide), 0)
            per = 3
            for base in range(0, heads // PAIR, per):
                strips = range(base, min(base + per, heads // PAIR))
                scores = [_dot(keys, q_s[n], 1, 1) for n in strips]
                weights, keeps = [], []
                for n, s in zip(strips, scores):
                    if masked:
                        s = jnp.where(ok, s, HIDDEN)
                    old = top_s[n]
                    top = jnp.maximum(old, s.max(axis=0, keepdims=True))
                    top_s[n] = top
                    weights.append(jnp.exp2((s - top) * e).astype(BF16))
                    keeps.append(jnp.exp2((old - top) * e))
                for n, p, keep in zip(strips, weights, keeps):
                    mix_s[n] = mix_s[n] * keep + _dot(values, p)

        lax.fori_loop(0, b, lambda j, _: block(j, False), None)
        block(b, True)
        for n in range(heads // PAIR):
            out = mix_s[n, :HEAD, :] * (1 / mix_s[n, HEAD : HEAD + 1, :])
            for i in range(PAIR):
                at = (n * PAIR + i) * HEAD
                seen_s[:, at : at + HEAD] = out[:, i * BLOCK : (i + 1) * BLOCK].T.astype(BF16)

    def project_block(b):
        first_tile = b * tiles
        def norm(at):
            total = jnp.zeros((at.size, 1), F32)
            for n in range(0, deep, unit):
                part = xa[at, n : n + unit].astype(F32)
                total += jnp.sum(part * part, axis=1, keepdims=True)
            scale = lax.rsqrt(total / deep + 1e-6)
            for n in range(0, deep, unit):
                part = xa[at, n : n + unit].astype(F32)
                xa[at, n : n + unit] = (part * scale * gains[n : n + unit].astype(F32)[None]).astype(BF16)
        @pl.when(b == 0)
        def _():
            gain_copy.wait()
        for n, c in enumerate(x_copies(b)):
            c.wait()
            passes(norm, 16, n * (BLOCK // PARTS), BLOCK // PARTS)

        qacc[...] = jnp.zeros(qacc.shape, F32)
        kvacc[...] = jnp.zeros(kvacc.shape, F32)

        @pl.when(b == 0)
        def _():
            for c in (*kv_copies, table_copy):
                c.wait()

        def project(i, _):
            g = first_tile + i

            @pl.when(i < depth_tiles - 2)
            def _():
                start_wq(b, i + 2)
            for n in range(2):
                @pl.when(i == depth_tiles - 2 + n)
                def _():
                    start_wo(b, n)
            slot = wait_tile(g)
            at = pl.ds(pl.multiple_of(i * unit, unit), unit)
            a = xa[:, at]
            for n in range(0, unit, 512):
                qacc[:, n : n + 512] += _dot(a, wbuf[slot, :, n : n + 512])
            kvacc[...] += _dot(a, wkv[at, :])
        lax.fori_loop(0, depth_tiles, project, None)

        @pl.when(b < blocks - 1)
        def _():
            for c in x_copies(b + 1):
                c.start()

    def rest_of_block(b):
        first_tile = b * tiles
        at = pl.ds(pl.multiple_of(b * BLOCK, BLOCK), BLOCK)
        cos, sin = table[0, at, :], table[1, at, :]

        def turned(t):
            t = t.astype(BF16).astype(F32)
            return (t * cos + pltpu.roll(t, HEAD // 2, 1) * sin).astype(BF16)
        for n in range(heads):
            i = n % PAIR
            q_s[n // PAIR, i * BLOCK : (i + 1) * BLOCK, :] = turned(qacc[:, n * HEAD : (n + 1) * HEAD])
        k_s[b] = turned(kvacc[:, :HEAD])
        vt_s[b, :HEAD, :] = kvacc[:, HEAD:].T.astype(BF16)
        vt_s[b, HEAD:, :] = jnp.ones((vt_s.shape[1] - HEAD, BLOCK), BF16)
        attend(b)

        for i, (give, j) in enumerate(ORDER):
            if i + 2 < len(ORDER):
                start_wo(b, i + 2)
            else:
                @pl.when(b < blocks - 1)
                def _():
                    start_wq(b + 1, i + 2 - len(ORDER))
            slot = wait_tile(first_tile + depth_tiles + i)
            if give:
                @pl.when(b > 0)
                def _():
                    d_copy(j).wait_send()
                for n in range(0, unit, 512):
                    dsend[j, :, n : n + 512] = _dot(seen_s[...], wbuf[slot, :, n : n + 512]).astype(BF16)

                @pl.when(b > 0)
                def _():
                    pl.semaphore_wait(d_free.at[j], 1)
                d_copy(j).start()
                continue
            d_copy(j).wait_recv()
            if j == 0:
                @pl.when(b > 0)
                def _():
                    for c in r1_copies:
                        c.wait_send()
            for n in range(0, unit, 512):
                value = _dot(seen_s[...], wbuf[slot, :, n : n + 512]) + drecv[j, :, n : n + 512].astype(F32)
                if j == 0:
                    r1s[:, n : n + 512] = value.astype(BF16)
                else:
                    own_s[j - 1, :, n : n + 512] = value

            @pl.when(b < blocks - 1)
            def _():
                signal(d_free.at[j], partner)
            if j == 0:
                @pl.when(b > 0)
                def _():
                    for n in range(2):
                        pl.semaphore_wait(r1_free.at[n], 1)
                for c in r1_copies:
                    c.start()

    for c in (*x_copies(0), gain_copy):
        c.start()
    barrier = pltpu.get_barrier_semaphore()
    for peer in (left, right, partner):
        pl.semaphore_signal(barrier, inc=1, device_id={axis: peer}, device_id_type=MESH)
    start_wq(0, 0)
    start_wq(0, 1)
    for c in (*kv_copies, table_copy):
        c.start()

    def stages(t, which):
        for back, stage in which:
            b = t - back

            end = last - 1 if stage is fourth_arrived else last if stage in (fourth, fourth_rest) else blocks

            @pl.when((b >= 0) & (b < end))
            def _():
                stage(b)

    def step(t, _):
        @pl.when(t < blocks)
        def _():
            project_block(t)

        @pl.when(t == 0)
        def _():
            pl.semaphore_wait(barrier, 3)
        stages(t, ((1, third),))

        @pl.when(t < blocks)
        def _():
            rest_of_block(t)
        stages(t, ((2, fourth_arrived), (1, fourth), (0, second), (1, fourth_rest)))

        @pl.when(t == last)
        def _():
            fourth_arrived(last - 1)
    lax.fori_loop(0, blocks + 1, step, None)

    for j in range(RING):
        d_copy(j).wait_send()
    for c in (*r1_copies, *r2_copies, *a2_copies(last - 1), *(p_copy(last - 1, n) for n in range(3))):
        c.wait_send()
    y_copy(last).wait()
    theirs = y_ref.at[pl.ds(0, last * BLOCK), pl.ds(0, RING * unit)]
    pltpu.make_async_copy(theirs, theirs, p_rs).wait()


def _copy_rows(first, count, *refs):
    staged_ref, (y_ref, bufs, ins, outs) = refs[0], refs[-4:]
    size = bufs.shape[1]
    rows = [pl.ds((first + i) * size, size) for i in range(count)]
    loads = [pltpu.make_async_copy(staged_ref.at[at, :], bufs.at[i % COPIES], ins.at[i % COPIES]) for i, at in enumerate(rows)]
    stores = [pltpu.make_async_copy(bufs.at[i % COPIES], y_ref.at[at, :], outs.at[i % COPIES]) for i, at in enumerate(rows)]
    ahead = COPIES // 2
    for i in range(min(ahead, count)):
        loads[i].start()
    for i in range(count):
        loads[i].wait()
        stores[i].start()
        j = i + ahead
        if j < count:
            if j >= COPIES:
                stores[j - COPIES].wait()
            loads[j].start()
    for i in range(max(count - COPIES, 0), count):
        stores[i].wait()


def _rows(staged, first, count, y=None, work=0):
    rows, deep = staged.shape
    size = BLOCK // 2
    given = [staged] if y is None else [staged, y]
    hbm, dma = pl.BlockSpec(memory_space=pl.ANY), pltpu.SemaphoreType.DMA
    return pl.pallas_call(
        functools.partial(_copy_rows, first, count),
        in_specs=[hbm] * len(given),
        out_specs=hbm,
        out_shape=jax.ShapeDtypeStruct(staged.shape, staged.dtype),
        input_output_aliases={} if y is None else {1: 0},
        scratch_shapes=[pltpu.VMEM((COPIES, size, deep), BF16), dma((COPIES,)), dma((COPIES,))],
        compiler_params=pltpu.CompilerParams(vmem_limit_bytes=40 * 2**20),
        cost_estimate=pl.CostEstimate(flops=count * work, bytes_accessed=count * size * deep * 4, transcendentals=0),
    )(*given)


def _last_block(axis, *refs):
    pieces, (y_ref, sems) = refs[1:-2], refs[-2:]
    unit = pieces[0].shape[1]
    start = y_ref.shape[0] - BLOCK
    me = lax.axis_index(axis)
    chip, core = me // 2, me % 2
    copies = []
    for n, piece in enumerate(pieces):
        k, part = n // 5, n % 5
        place = (core + k) % 2
        away = (0, RING - 1, 1, 2, 2)[part]
        at = pl.ds(pl.multiple_of(((chip + away) % RING) * (2 * unit) + place * unit, unit), unit)
        size = piece.shape[0]
        copies.append(pltpu.make_async_copy(piece, y_ref.at[pl.ds(start + (size if part == 4 else 0), size), at], sems.at[n]))
    for c in copies:
        c.start()
    for c in copies:
        c.wait()


def solution(mesh):
    axis = mesh.axis_names[1]
    group = mesh.shape[axis]

    def step(x, gain, wq, wk, wv, wo):
        rows, deep = x.shape
        unit = deep // group
        blocks = rows // BLOCK
        heads = unit // HEAD
        part = HEAD // 2
        angle = np.arange(rows, dtype=np.float32)[:, None] * np.float32(THETA) ** (-np.arange(part, dtype=np.float32) / np.float32(part))
        angle = angle.astype(np.float64)
        cos, sin = (jnp.asarray(f(angle).astype(np.float32)) for f in (np.cos, np.sin))
        table = jnp.stack([jnp.concatenate([cos, cos], 1), jnp.concatenate([-sin, sin], 1)])
        vmem, hbm = pl.BlockSpec(memory_space=pltpu.VMEM), pl.BlockSpec(memory_space=pl.ANY)
        dma, regular = pltpu.SemaphoreType.DMA, pltpu.SemaphoreType.REGULAR
        strips = heads // PAIR
        staged, mine = pl.pallas_call(
            functools.partial(_layer, axis),
            out_shape=[jax.ShapeDtypeStruct((rows, deep), BF16), jax.ShapeDtypeStruct((BLOCK, unit), BF16)],
            in_specs=[hbm] * 7,
            out_specs=[hbm, hbm],
            scratch_shapes=[
                pltpu.VMEM((BLOCK, deep), BF16),
                pltpu.VMEM((2, rows, HEAD), F32),
                pltpu.VMEM((deep,), BF16),
                pltpu.VMEM((BUFFERS, unit, unit), BF16),
                pltpu.VMEM((deep, 2 * HEAD), BF16),
                pltpu.VMEM((BLOCK, unit), F32),
                pltpu.VMEM((BLOCK, 2 * HEAD), F32),
                pltpu.VMEM((strips, PAIR * BLOCK, HEAD), BF16),
                pltpu.VMEM((blocks, BLOCK, HEAD), BF16),
                pltpu.VMEM((blocks, HEAD + 16, BLOCK), BF16),
                pltpu.VMEM((strips, 1, PAIR * BLOCK), F32),
                pltpu.VMEM((strips, HEAD + 16, PAIR * BLOCK), F32),
                pltpu.VMEM((BLOCK, unit), BF16),
                pltpu.VMEM((RING - 1, BLOCK, unit), F32),
                pltpu.VMEM((RING, BLOCK, unit), BF16),
                pltpu.VMEM((RING, BLOCK, unit), BF16),
                pltpu.VMEM((BLOCK, unit), BF16),
                pltpu.VMEM((BLOCK, unit), BF16),
                pltpu.VMEM((2, BLOCK, unit), BF16),
                pltpu.VMEM((2, BLOCK, unit), BF16),
                pltpu.VMEM((BLOCK, unit), BF16),
                pltpu.VMEM((BLOCK, unit), BF16),
                dma((BUFFERS,)), dma((PARTS,)), dma, dma, dma((2,)), dma, dma,
                dma((RING,)), dma((RING,)), regular((RING,)),
                dma((2,)), dma((2,)), regular((2,)),
                dma((2,)), dma((2,)), regular((2,)),
                dma((3,)), dma((2, 2)),
                dma((4,)), dma((2, 4)),
                dma((3,)), dma,
            ],
            compiler_params=pltpu.CompilerParams(collective_id=0, has_side_effects=True, vmem_limit_bytes=VMEM),
        )(x, gain, table, wq, wk, wv, wo)

        def hop(value, chips, cores):
            return lax.ppermute(value, axis, [(t, (t + 2 * chips) % group // 2 * 2 + (t + cores) % 2) for t in range(group)])

        count = 2 * (rows // BLOCK - 1)
        early = count * FIRST // 14
        half = BLOCK // 2
        from_left, from_right, beside = hop(mine, 1, 0), hop(mine, -1, 0), hop(mine, 0, 1)
        y = _rows(staged, 0, early, work=WORK)
        y, from_left, from_right = lax.optimization_barrier((y, from_left, from_right))
        upper, lower = hop(from_left[:half], 1, 0), hop(from_right[half:], -1, 0)
        others = [beside, hop(from_left, 0, 1), hop(from_right, 0, 1)]
        y = _rows(staged, early, count - early, y, work=WORK)
        y, upper, lower = lax.optimization_barrier((y, upper, lower))
        others += [hop(upper, 0, 1), hop(lower, 0, 1)]
        pieces = [mine, from_left, from_right, upper, lower, *others]
        return pl.pallas_call(
            functools.partial(_last_block, axis),
            out_shape=jax.ShapeDtypeStruct((rows, deep), BF16),
            in_specs=[hbm] + [vmem] * len(pieces),
            out_specs=hbm,
            input_output_aliases={0: 0},
            scratch_shapes=[dma((len(pieces),))],
        )(y, *pieces)

    tokens, columns = P(mesh.axis_names[0], None), P(None, axis)
    return jax.shard_map(
        step,
        mesh=mesh,
        in_specs=(tokens, P(None), columns, columns, columns, P(axis, None)),
        out_specs=tokens,
        check_vma=False,
    )
```

```python
import functools

import jax
import jax.numpy as jnp
import numpy as np
from jax import lax
from jax.experimental import pallas as pl
from jax.experimental.pallas import tpu as pltpu
from jax.sharding import PartitionSpec as P

HEAD = 128
THETA = 10000
NEG = -1e30
HIDDEN = 2 * NEG
LOG2E = 1.4426950408889634
VMEM = 66_900_000
BLOCK = 256
PAIR = 2
RING = 4
BUFFERS = 3
FIRST = 19
WORK = 500_000_000
SPLIT = 5
COPIES = 20
PARTS = 4
AWAY = (2, 1, RING - 1, 0)
ORDER = ((True, 0), (True, 1), (False, 0), (True, 2), (False, 1), (True, 3), (False, 2), (False, 3))
MESH = pl.DeviceIdType.MESH
F32, BF16 = jnp.float32, jnp.bfloat16


def _dot(a, b, ca=1, cb=0):
    return lax.dot_general(a, b, (((ca,), (cb,)), ((), ())), preferred_element_type=F32)


def _layer(axis, x_ref, gain_ref, table_ref, wq_ref, wk_ref, wv_ref, wo_ref, y_ref, last_ref, xa, table, gains, wbuf, wkv, qacc, kvacc, q_s, k_s, vt_s, top_s,
           mix_s, seen_s, own_s, dsend, drecv, r1s, r1r, r2s, r2r, ys, xres, wsem, xsem, tsem, gsem, kvsem, ressem, ysem, d_ss, d_rs, d_free, r1_ss, r1_rs,
           r1_free, r2_ss, r2_rs, r2_free, a1_ss, a1_rs, a2_ss, a2_rs, p_ss, p_rs):
    rows, deep = x_ref.shape
    unit = r1s.shape[1]
    blocks = rows // BLOCK
    last = blocks - 1
    heads = unit // HEAD
    half = BLOCK // 2
    depth_tiles = deep // unit
    tiles = depth_tiles + 2 * RING
    me = lax.axis_index(axis)
    chip, core = me // 2, me % 2
    other = 1 - core
    right = ((chip + 1) % RING) * 2 + core
    left = ((chip + RING - 1) % RING) * 2 + core
    partner = chip * 2 + other
    upper, lower = pl.ds(0, half), pl.ds(half, half)

    def remote(src, dst, ss, rs, peer):
        return pltpu.make_async_remote_copy(src_ref=src, dst_ref=dst, send_sem=ss, recv_sem=rs, device_id={axis: peer}, device_id_type=MESH)

    def signal(sem, peer):
        pl.semaphore_signal(sem, inc=1, device_id={axis: peer}, device_id_type=MESH)

    def columns(away, k):
        return pl.ds(pl.multiple_of(((chip + away) % RING) * (2 * unit) + k * unit, unit), unit)

    def yref(b, part, away):
        start, size = part
        return y_ref.at[pl.ds(pl.multiple_of(b * BLOCK + start, half // 2), size), columns(away, core)]

    whole = (0, BLOCK)

    def start_wq(b, i):
        slot = (b * tiles + i) % BUFFERS
        at = pl.ds(pl.multiple_of(i * unit, unit), unit)
        pltpu.make_async_copy(wq_ref.at[at, :], wbuf.at[slot], wsem.at[slot]).start()

    def start_wo(b, i):
        slot = (b * tiles + depth_tiles + i) % BUFFERS
        give, j = ORDER[i]
        pltpu.make_async_copy(wo_ref.at[:, columns(AWAY[j], other if give else core)], wbuf.at[slot], wsem.at[slot]).start()

    def wait_tile(g):
        slot = g % BUFFERS
        pltpu.make_async_copy(wq_ref.at[pl.ds(0, unit), :], wbuf.at[slot], wsem.at[slot]).wait()
        return slot

    def x_copies(b):
        made = []
        for n in range(PARTS):
            size = BLOCK // PARTS
            made.append(pltpu.make_async_copy(x_ref.at[pl.ds(pl.multiple_of(b * BLOCK + n * size, size), size), :], xa.at[pl.ds(n * size, size), :],
                                              xsem.at[n]))
        return made

    table_copy = pltpu.make_async_copy(table_ref, table, tsem)
    gain_copy = pltpu.make_async_copy(gain_ref, gains, gsem)
    kv_copies = [pltpu.make_async_copy(w, wkv.at[:, pl.ds(n * HEAD, HEAD)], kvsem.at[n]) for n, w in enumerate((wk_ref, wv_ref))]

    def d_copy(j):
        return remote(dsend.at[j], drecv.at[j], d_ss.at[j], d_rs.at[j], partner)

    r1_copies = [remote(r1s.at[upper], r1r.at[upper], r1_ss.at[0], r1_rs.at[0], left),
                 remote(r1s.at[lower], r1r.at[lower], r1_ss.at[1], r1_rs.at[1], right)]
    def r2_copy(n, part):
        at = (upper, lower)[part]
        return remote(r2s.at[n, at], r2r.at[n, at], r2_ss.at[2 * n + part], r2_rs.at[2 * n + part], (left, right)[n])

    r2_alone, r2_added = (r2_copy(0, 1), r2_copy(1, 0)), (r2_copy(0, 0), r2_copy(1, 1))
    r2_copies = (*r2_alone, *r2_added)

    def a1_copies(b):
        p = b % 2
        mine = yref(b, whole, 0)
        return [remote(ys, mine, a1_ss.at[0], a1_rs.at[p, 0], left), remote(ys, mine, a1_ss.at[1], a1_rs.at[p, 1], right),
                remote(ys, mine, a1_ss.at[2], p_rs, partner)]

    def a1_arrived(b):
        p = b % 2
        for n in range(2):
            remote(ys, yref(b, whole, 0), a1_ss.at[n], a1_rs.at[p, n], left).wait_recv()

    def a2_copies(b, parts=(0, 1)):
        p, made = b % 2, []
        for n in parts:
            for to, away, start, peer in ((0, 1, half, left), (1, RING - 1, 0, right)):
                piece = yref(b, (start + n * (half // 2), half // 2), away)
                made.append(remote(piece, piece, a2_ss.at[2 * n + to], a2_rs.at[p, 2 * n + to], peer))
        return made

    def p_copy(b, n):
        away = (1, RING - 1, 2)[n]
        return remote(yref(b, whole, away), yref(b, whole, away), p_ss.at[n], p_rs, partner)

    def y_copy(b):
        return pltpu.make_async_copy(ys, yref(b, whole, 0), ysem)

    def res_copy(b):
        return pltpu.make_async_copy(x_ref.at[pl.ds(pl.multiple_of(b * BLOCK, BLOCK), BLOCK), columns(0, core)], xres, ressem)

    def passes(body, step=32, start=0, size=BLOCK):
        def one(r, _):
            body(pl.ds(pl.multiple_of(start + r * step, step), step))
        lax.fori_loop(0, size // step, one, None)

    def fourth_arrived(b):
        for c in a2_copies(b):
            c.wait_recv()

        @pl.when(b > 0)
        def _():
            p_copy(b, 2).wait_send()
        p_copy(b, 2).start()

    def fourth(b):
        a1_arrived(b)

        @pl.when(b > 0)
        def _():
            for c in (*a2_copies(b), p_copy(b, 0), p_copy(b, 1)):
                c.wait_send()
        for c in (*a2_copies(b, (0,)), p_copy(b, 0), p_copy(b, 1)):
            c.start()

    def fourth_rest(b):
        for c in a2_copies(b, (1,)):
            c.start()

    def third(b):
        res_copy(b).start()
        for c in r2_copies:
            c.wait_recv()

        @pl.when(b > 0)
        def _():
            for c in a1_copies(b):
                c.wait_send()
            y_copy(b).wait()
        res_copy(b).wait()

        def finish(at):
            total = own_s[2, at, :] + r2r[0, at, :].astype(F32) + r2r[1, at, :].astype(F32)
            ys[at, :] = (xres[at, :].astype(F32) + total).astype(BF16)
        passes(finish)

        @pl.when(b < blocks - 1)
        def _():
            signal(r2_free.at[0], right)
            signal(r2_free.at[1], left)

        @pl.when(b < last)
        def _():
            for c in a1_copies(b):
                c.start()
            y_copy(b).start()

        @pl.when(b == last)
        def _():
            pltpu.make_async_copy(ys, last_ref, ysem).start()

    def second(b):
        for c in r1_copies:
            c.wait_recv()

        @pl.when(b > 0)
        def _():
            for c in r2_added:
                c.wait_send()

        def add(at):
            r2s[0, at, :] = (own_s[1, at, :] + r1r[at, :].astype(F32)).astype(BF16)
        passes(add, size=half)

        def add(at):
            r2s[1, at, :] = (own_s[0, at, :] + r1r[at, :].astype(F32)).astype(BF16)
        passes(add, start=half, size=half)

        @pl.when(b < blocks - 1)
        def _():
            signal(r1_free.at[0], right)
            signal(r1_free.at[1], left)
        @pl.when(b > 0)
        def _():
            for n in range(2):
                pl.semaphore_wait(r2_free.at[n], 1)
            for c in r2_alone:
                c.start()
        for c in r2_added:
            c.start()

    def attend(b):
        e = HEAD**-0.5 * LOG2E
        wide = PAIR * BLOCK
        for n in range(heads // PAIR):
            top_s[n] = jnp.full((1, wide), NEG, F32)
            mix_s[n] = jnp.zeros(mix_s.shape[1:], F32)

        def block(j, masked):
            keys = k_s[j]
            values = vt_s[j]
            if masked:
                ok = lax.rem(lax.broadcasted_iota(jnp.int32, (BLOCK, wide), 1), BLOCK) >= lax.broadcasted_iota(jnp.int32, (BLOCK, wide), 0)
            per = 3
            for base in range(0, heads // PAIR, per):
                strips = range(base, min(base + per, heads // PAIR))
                scores = [_dot(keys, q_s[n], 1, 1) for n in strips]
                weights, keeps = [], []
                for n, s in zip(strips, scores):
                    if masked:
                        s = jnp.where(ok, s, HIDDEN)
                    old = top_s[n]
                    top = jnp.maximum(old, s.max(axis=0, keepdims=True))
                    top_s[n] = top
                    weights.append(jnp.exp2((s - top) * e).astype(BF16))
                    keeps.append(jnp.exp2((old - top) * e))
                for n, p, keep in zip(strips, weights, keeps):
                    mix_s[n] = mix_s[n] * keep + _dot(values, p)

        lax.fori_loop(0, b, lambda j, _: block(j, False), None)
        block(b, True)
        for n in range(heads // PAIR):
            out = mix_s[n, :HEAD, :] * (1 / mix_s[n, HEAD : HEAD + 1, :])
            for i in range(PAIR):
                at = (n * PAIR + i) * HEAD
                seen_s[:, at : at + HEAD] = out[:, i * BLOCK : (i + 1) * BLOCK].T.astype(BF16)

    def project_block(b):
        first_tile = b * tiles
        def norm(at):
            total = jnp.zeros((at.size, 1), F32)
            for n in range(0, deep, unit):
                part = xa[at, n : n + unit].astype(F32)
                total += jnp.sum(part * part, axis=1, keepdims=True)
            scale = lax.rsqrt(total / deep + 1e-6)
            for n in range(0, deep, unit):
                part = xa[at, n : n + unit].astype(F32)
                xa[at, n : n + unit] = (part * scale * gains[n : n + unit].astype(F32)[None]).astype(BF16)
        @pl.when(b == 0)
        def _():
            gain_copy.wait()
        for n, c in enumerate(x_copies(b)):
            c.wait()
            passes(norm, 16, n * (BLOCK // PARTS), BLOCK // PARTS)

        qacc[...] = jnp.zeros(qacc.shape, F32)
        kvacc[...] = jnp.zeros(kvacc.shape, F32)

        @pl.when(b == 0)
        def _():
            for c in (*kv_copies, table_copy):
                c.wait()
            pl.semaphore_wait(barrier, 3)

        def project(i, _):
            @pl.when((i == SPLIT) & (b == 1))
            def _():
                third(0)
            g = first_tile + i

            @pl.when(i < depth_tiles - 2)
            def _():
                start_wq(b, i + 2)
            for n in range(2):
                @pl.when(i == depth_tiles - 2 + n)
                def _():
                    start_wo(b, n)
            slot = wait_tile(g)
            at = pl.ds(pl.multiple_of(i * unit, unit), unit)
            a = xa[:, at]
            for n in range(0, unit, 512):
                qacc[:, n : n + 512] += _dot(a, wbuf[slot, :, n : n + 512])
            kvacc[...] += _dot(a, wkv[at, :])
        lax.fori_loop(0, depth_tiles, project, None)

        @pl.when(b < blocks - 1)
        def _():
            for c in x_copies(b + 1):
                c.start()

    def rest_of_block(b):
        first_tile = b * tiles
        at = pl.ds(pl.multiple_of(b * BLOCK, BLOCK), BLOCK)
        cos, sin = table[0, at, :], table[1, at, :]

        def turned(t):
            t = t.astype(BF16).astype(F32)
            return (t * cos + pltpu.roll(t, HEAD // 2, 1) * sin).astype(BF16)
        for n in range(heads):
            i = n % PAIR
            q_s[n // PAIR, i * BLOCK : (i + 1) * BLOCK, :] = turned(qacc[:, n * HEAD : (n + 1) * HEAD])
        k_s[b] = turned(kvacc[:, :HEAD])
        vt_s[b, :HEAD, :] = kvacc[:, HEAD:].T.astype(BF16)
        vt_s[b, HEAD:, :] = jnp.ones((vt_s.shape[1] - HEAD, BLOCK), BF16)
        attend(b)

        for i, (give, j) in enumerate(ORDER):
            if i + 2 < len(ORDER):
                start_wo(b, i + 2)
            else:
                @pl.when(b < blocks - 1)
                def _():
                    start_wq(b + 1, i + 2 - len(ORDER))
            slot = wait_tile(first_tile + depth_tiles + i)
            if give:
                @pl.when(b > 0)
                def _():
                    d_copy(j).wait_send()
                for n in range(0, unit, 512):
                    dsend[j, :, n : n + 512] = _dot(seen_s[...], wbuf[slot, :, n : n + 512]).astype(BF16)

                @pl.when(b > 0)
                def _():
                    pl.semaphore_wait(d_free.at[j], 1)
                d_copy(j).start()
                continue
            d_copy(j).wait_recv()
            if j < 3:
                @pl.when(b > 0)
                def _():
                    for c in (r1_copies, r2_alone[1:], r2_alone[:1])[j]:
                        c.wait_send()
            for n in range(0, unit, 512):
                value = _dot(seen_s[...], wbuf[slot, :, n : n + 512]) + drecv[j, :, n : n + 512].astype(F32)
                if j == 0:
                    r1s[:, n : n + 512] = value.astype(BF16)
                elif j == 1:
                    r2s[1, upper, n : n + 512] = value[:half].astype(BF16)
                    own_s[0, lower, n : n + 512] = value[half:]
                elif j == 2:
                    r2s[0, lower, n : n + 512] = value[half:].astype(BF16)
                    own_s[1, upper, n : n + 512] = value[:half]
                else:
                    own_s[2, :, n : n + 512] = value

            @pl.when(b < blocks - 1)
            def _():
                signal(d_free.at[j], partner)
            if j == 0:
                @pl.when(b > 0)
                def _():
                    for n in range(2):
                        pl.semaphore_wait(r1_free.at[n], 1)
                for c in r1_copies:
                    c.start()
            elif j < 3:
                c = r2_alone[2 - j]

                @pl.when(b == 0)
                def _():
                    c.start()

    for c in (*x_copies(0), gain_copy):
        c.start()
    barrier = pltpu.get_barrier_semaphore()
    for peer in (left, right, partner):
        pl.semaphore_signal(barrier, inc=1, device_id={axis: peer}, device_id_type=MESH)
    start_wq(0, 0)
    start_wq(0, 1)
    for c in (*kv_copies, table_copy):
        c.start()

    def stages(t, which):
        for back, stage in which:
            b = t - back

            end = last - 1 if stage is fourth_arrived else last if stage is fourth else blocks

            @pl.when((b >= 0) & (b < end))
            def _():
                stage(b)

    def step(t, _):
        @pl.when(t < blocks)
        def _():
            project_block(t)

        @pl.when((t > 1) & (t < blocks))
        def _():
            fourth_rest(t - 2)

        @pl.when(t == blocks)
        def _():
            fourth_arrived(last - 1)

        @pl.when(t > 1)
        def _():
            third(t - 1)

        @pl.when(t < blocks)
        def _():
            rest_of_block(t)
        stages(t, ((2, fourth_arrived), (1, fourth)))

        @pl.when(t == last)
        def _():
            fourth_rest(last - 1)
        stages(t, ((0, second),))
    lax.fori_loop(0, blocks + 1, step, None)

    for j in range(RING):
        d_copy(j).wait_send()
    for c in (*r1_copies, *r2_copies, *a2_copies(last - 1), *(p_copy(last - 1, n) for n in range(3))):
        c.wait_send()
    y_copy(last).wait()
    theirs = y_ref.at[pl.ds(0, last * BLOCK), pl.ds(0, RING * unit)]
    pltpu.make_async_copy(theirs, theirs, p_rs).wait()


def _copy_rows(first, count, *refs):
    staged_ref, (y_ref, bufs, ins, outs) = refs[0], refs[-4:]
    size = bufs.shape[1]
    rows = [pl.ds((first + i) * size, size) for i in range(count)]
    loads = [pltpu.make_async_copy(staged_ref.at[at, :], bufs.at[i % COPIES], ins.at[i % COPIES]) for i, at in enumerate(rows)]
    stores = [pltpu.make_async_copy(bufs.at[i % COPIES], y_ref.at[at, :], outs.at[i % COPIES]) for i, at in enumerate(rows)]
    ahead = COPIES // 2
    for i in range(min(ahead, count)):
        loads[i].start()
    for i in range(count):
        loads[i].wait()
        stores[i].start()
        j = i + ahead
        if j < count:
            if j >= COPIES:
                stores[j - COPIES].wait()
            loads[j].start()
    for i in range(max(count - COPIES, 0), count):
        stores[i].wait()


def _rows(staged, first, count, y=None, work=0):
    rows, deep = staged.shape
    size = BLOCK // 8
    given = [staged] if y is None else [staged, y]
    hbm, dma = pl.BlockSpec(memory_space=pl.ANY), pltpu.SemaphoreType.DMA
    return pl.pallas_call(
        functools.partial(_copy_rows, first, count),
        in_specs=[hbm] * len(given),
        out_specs=hbm,
        out_shape=jax.ShapeDtypeStruct(staged.shape, staged.dtype),
        input_output_aliases={} if y is None else {1: 0},
        scratch_shapes=[pltpu.VMEM((COPIES, size, deep), BF16), dma((COPIES,)), dma((COPIES,))],
        compiler_params=pltpu.CompilerParams(vmem_limit_bytes=40 * 2**20),
        cost_estimate=pl.CostEstimate(flops=count * work, bytes_accessed=count * size * deep * 4, transcendentals=0),
    )(*given)


def _place(axis, marks, *refs):
    pieces, (y_ref, buf, ins, outs) = refs[1:-4], refs[-4:]
    unit = buf.shape[2]
    start = y_ref.shape[0] - BLOCK
    me = lax.axis_index(axis)
    chip, core = me // 2, me % 2
    loads, stores = [], []
    for n, (piece, (k, away, row)) in enumerate(zip(pieces, marks)):
        at = pl.ds(pl.multiple_of(((chip + away) % RING) * (2 * unit) + ((core + k) % 2) * unit, unit), unit)
        size = piece.shape[0]
        vmem = buf.at[n, pl.ds(0, size), :]
        loads.append(pltpu.make_async_copy(piece, vmem, ins.at[n]))
        stores.append(pltpu.make_async_copy(vmem, y_ref.at[pl.ds(start + row, size), at], outs.at[n]))
    for c in loads:
        c.start()
    for c, out in zip(loads, stores):
        c.wait()
        out.start()
    for c in stores:
        c.wait()


def _placed(axis, y, marked):
    marks, pieces = zip(*marked)
    hbm, dma = pl.BlockSpec(memory_space=pl.ANY), pltpu.SemaphoreType.DMA
    tall, unit = max(p.shape[0] for p in pieces), pieces[0].shape[1]
    return pl.pallas_call(
        functools.partial(_place, axis, marks),
        out_shape=jax.ShapeDtypeStruct(y.shape, y.dtype),
        in_specs=[hbm] * (1 + len(pieces)),
        out_specs=hbm,
        input_output_aliases={0: 0},
        scratch_shapes=[pltpu.VMEM((len(pieces), tall, unit), BF16), dma((len(pieces),)), dma((len(pieces),))],
        cost_estimate=pl.CostEstimate(flops=4 * WORK, bytes_accessed=4 * sum(p.size for p in pieces), transcendentals=0),
    )(y, *pieces)


def solution(mesh):
    axis = mesh.axis_names[1]
    group = mesh.shape[axis]

    def step(x, gain, wq, wk, wv, wo):
        rows, deep = x.shape
        unit = deep // group
        blocks = rows // BLOCK
        heads = unit // HEAD
        part = HEAD // 2
        angle = np.arange(rows, dtype=np.float32)[:, None] * np.float32(THETA) ** (-np.arange(part, dtype=np.float32) / np.float32(part))
        angle = angle.astype(np.float64)
        cos, sin = (jnp.asarray(f(angle).astype(np.float32)) for f in (np.cos, np.sin))
        table = jnp.stack([jnp.concatenate([cos, cos], 1), jnp.concatenate([-sin, sin], 1)])
        vmem, hbm = pl.BlockSpec(memory_space=pltpu.VMEM), pl.BlockSpec(memory_space=pl.ANY)
        dma, regular = pltpu.SemaphoreType.DMA, pltpu.SemaphoreType.REGULAR
        strips = heads // PAIR
        staged, mine = pl.pallas_call(
            functools.partial(_layer, axis),
            out_shape=[jax.ShapeDtypeStruct((rows, deep), BF16), jax.ShapeDtypeStruct((BLOCK, unit), BF16)],
            in_specs=[hbm] * 7,
            out_specs=[hbm, hbm],
            scratch_shapes=[
                pltpu.VMEM((BLOCK, deep), BF16),
                pltpu.VMEM((2, rows, HEAD), F32),
                pltpu.VMEM((deep,), BF16),
                pltpu.VMEM((BUFFERS, unit, unit), BF16),
                pltpu.VMEM((deep, 2 * HEAD), BF16),
                pltpu.VMEM((BLOCK, unit), F32),
                pltpu.VMEM((BLOCK, 2 * HEAD), F32),
                pltpu.VMEM((strips, PAIR * BLOCK, HEAD), BF16),
                pltpu.VMEM((blocks, BLOCK, HEAD), BF16),
                pltpu.VMEM((blocks, HEAD + 16, BLOCK), BF16),
                pltpu.VMEM((strips, 1, PAIR * BLOCK), F32),
                pltpu.VMEM((strips, HEAD + 16, PAIR * BLOCK), F32),
                pltpu.VMEM((BLOCK, unit), BF16),
                pltpu.VMEM((RING - 1, BLOCK, unit), F32),
                pltpu.VMEM((RING, BLOCK, unit), BF16),
                pltpu.VMEM((RING, BLOCK, unit), BF16),
                pltpu.VMEM((BLOCK, unit), BF16),
                pltpu.VMEM((BLOCK, unit), BF16),
                pltpu.VMEM((2, BLOCK, unit), BF16),
                pltpu.VMEM((2, BLOCK, unit), BF16),
                pltpu.VMEM((BLOCK, unit), BF16),
                pltpu.VMEM((BLOCK, unit), BF16),
                dma((BUFFERS,)), dma((PARTS,)), dma, dma, dma((2,)), dma, dma,
                dma((RING,)), dma((RING,)), regular((RING,)),
                dma((2,)), dma((2,)), regular((2,)),
                dma((4,)), dma((4,)), regular((2,)),
                dma((3,)), dma((2, 2)),
                dma((4,)), dma((2, 4)),
                dma((3,)), dma,
            ],
            compiler_params=pltpu.CompilerParams(collective_id=0, has_side_effects=True, vmem_limit_bytes=VMEM),
        )(x, gain, table, wq, wk, wv, wo)

        def hop(value, chips, cores):
            return lax.ppermute(value, axis, [(t, (t + 2 * chips) % group // 2 * 2 + (t + cores) % 2) for t in range(group)])

        count = 8 * (rows // BLOCK - 1)
        early = count * FIRST // 28
        half = BLOCK // 2
        from_left, from_right, beside = hop(mine, 1, 0), hop(mine, -1, 0), hop(mine, 0, 1)
        y = _rows(staged, 0, early, work=WORK)
        y, from_left, from_right = lax.optimization_barrier((y, from_left, from_right))
        upper, lower = hop(from_left[:half], 1, 0), hop(from_right[half:], -1, 0)
        marked = [((0, 0, 0), mine), ((1, 0, 0), beside), ((0, RING - 1, 0), from_left), ((0, 1, 0), from_right),
                  ((1, RING - 1, 0), hop(from_left, 0, 1)), ((1, 1, 0), hop(from_right, 0, 1))]
        y = _rows(staged, early, count - early, y, work=WORK)
        y, upper, lower = lax.optimization_barrier((y, upper, lower))
        late = [((0, 2, 0), upper), ((0, 2, half), lower), ((1, 2, 0), hop(upper, 0, 1)), ((1, 2, half), hop(lower, 0, 1))]
        return _placed(axis, _placed(axis, y, marked), late)

    tokens, columns = P(mesh.axis_names[0], None), P(None, axis)
    return jax.shard_map(
        step,
        mesh=mesh,
        in_specs=(tokens, P(None), columns, columns, columns, P(axis, None)),
        out_specs=tokens,
        check_vma=False,
    )
```

```python
import functools

import jax
import jax.numpy as jnp
import numpy as np
from jax import lax
from jax.experimental import pallas as pl
from jax.experimental.pallas import tpu as pltpu
from jax.sharding import PartitionSpec as P

HEAD = 128
THETA = 10000
NEG = -1e30
HIDDEN = 2 * NEG
LOG2E = 1.4426950408889634
VMEM = 66_900_000
BLOCK = 256
PAIR = 2
RING = 4
BUFFERS = 3
FIRST = 19
WORK = 500_000_000
SPLIT = 5
COPIES = 20
PARTS = 4
AWAY = (2, 1, RING - 1, 0)
ORDER = ((True, 0), (True, 1), (False, 0), (True, 2), (False, 1), (True, 3), (False, 2), (False, 3))
MESH = pl.DeviceIdType.MESH
F32, BF16 = jnp.float32, jnp.bfloat16


def _dot(a, b, ca=1, cb=0):
    return lax.dot_general(a, b, (((ca,), (cb,)), ((), ())), preferred_element_type=F32)


def _layer(axis, x_ref, gain_ref, table_ref, wq_ref, wk_ref, wv_ref, wo_ref, y_ref, last_ref, xa, table, gains, wbuf, wkv, qacc, kvacc, q_s, k_s, vt_s, top_s,
           mix_s, seen_s, own_s, dsend, drecv, r1s, r1r, r2s, r2r, ys, xres, wsem, xsem, tsem, gsem, kvsem, ressem, ysem, d_ss, d_rs, d_free, r1_ss, r1_rs,
           r1_free, r2_ss, r2_rs, r2_free, a1_ss, a1_rs, a2_ss, a2_rs, p_ss, p_rs):
    rows, deep = x_ref.shape
    unit = r1s.shape[1]
    blocks = rows // BLOCK
    last = blocks - 1
    heads = unit // HEAD
    half = BLOCK // 2
    depth_tiles = deep // unit
    tiles = depth_tiles + 2 * RING
    me = lax.axis_index(axis)
    chip, core = me // 2, me % 2
    other = 1 - core
    right = ((chip + 1) % RING) * 2 + core
    left = ((chip + RING - 1) % RING) * 2 + core
    partner = chip * 2 + other
    upper, lower = pl.ds(0, half), pl.ds(half, half)

    def remote(src, dst, ss, rs, peer):
        return pltpu.make_async_remote_copy(src_ref=src, dst_ref=dst, send_sem=ss, recv_sem=rs, device_id={axis: peer}, device_id_type=MESH)

    def signal(sem, peer):
        pl.semaphore_signal(sem, inc=1, device_id={axis: peer}, device_id_type=MESH)

    def columns(away, k):
        return pl.ds(pl.multiple_of(((chip + away) % RING) * (2 * unit) + k * unit, unit), unit)

    def yref(b, part, away):
        start, size = part
        return y_ref.at[pl.ds(pl.multiple_of(b * BLOCK + start, half // 2), size), columns(away, core)]

    whole = (0, BLOCK)

    def start_wq(b, i):
        slot = (b * tiles + i) % BUFFERS
        at = pl.ds(pl.multiple_of(i * unit, unit), unit)
        pltpu.make_async_copy(wq_ref.at[at, :], wbuf.at[slot], wsem.at[slot]).start()

    def start_wo(b, i):
        slot = (b * tiles + depth_tiles + i) % BUFFERS
        give, j = ORDER[i]
        pltpu.make_async_copy(wo_ref.at[:, columns(AWAY[j], other if give else core)], wbuf.at[slot], wsem.at[slot]).start()

    def wait_tile(g):
        slot = g % BUFFERS
        pltpu.make_async_copy(wq_ref.at[pl.ds(0, unit), :], wbuf.at[slot], wsem.at[slot]).wait()
        return slot

    def x_copies(b):
        made = []
        for n in range(PARTS):
            size = BLOCK // PARTS
            made.append(pltpu.make_async_copy(x_ref.at[pl.ds(pl.multiple_of(b * BLOCK + n * size, size), size), :], xa.at[pl.ds(n * size, size), :],
                                              xsem.at[n]))
        return made

    table_copy = pltpu.make_async_copy(table_ref, table, tsem)
    gain_copy = pltpu.make_async_copy(gain_ref, gains, gsem)
    kv_copies = [pltpu.make_async_copy(w, wkv.at[:, pl.ds(n * HEAD, HEAD)], kvsem.at[n]) for n, w in enumerate((wk_ref, wv_ref))]

    def d_copy(j):
        return remote(dsend.at[j], drecv.at[j], d_ss.at[j], d_rs.at[j], partner)

    r1_copies = [remote(r1s.at[upper], r1r.at[upper], r1_ss.at[0], r1_rs.at[0], left),
                 remote(r1s.at[lower], r1r.at[lower], r1_ss.at[1], r1_rs.at[1], right)]
    def r2_copy(n, part):
        at = (upper, lower)[part]
        return remote(r2s.at[n, at], r2r.at[n, at], r2_ss.at[2 * n + part], r2_rs.at[2 * n + part], (left, right)[n])

    r2_alone, r2_added = (r2_copy(0, 1), r2_copy(1, 0)), (r2_copy(0, 0), r2_copy(1, 1))
    r2_copies = (*r2_alone, *r2_added)

    def a1_copies(b):
        p = b % 2
        mine = yref(b, whole, 0)
        return [remote(ys, mine, a1_ss.at[0], a1_rs.at[p, 0], left), remote(ys, mine, a1_ss.at[1], a1_rs.at[p, 1], right),
                remote(ys, mine, a1_ss.at[2], p_rs, partner)]

    def a1_arrived(b):
        p = b % 2
        for n in range(2):
            remote(ys, yref(b, whole, 0), a1_ss.at[n], a1_rs.at[p, n], left).wait_recv()

    def a2_copies(b, parts=(0, 1)):
        p, made = b % 2, []
        for n in parts:
            for to, away, start, peer in ((0, 1, half, left), (1, RING - 1, 0, right)):
                piece = yref(b, (start + n * (half // 2), half // 2), away)
                made.append(remote(piece, piece, a2_ss.at[2 * n + to], a2_rs.at[p, 2 * n + to], peer))
        return made

    def p_copy(b, n):
        away = (1, RING - 1, 2)[n]
        return remote(yref(b, whole, away), yref(b, whole, away), p_ss.at[n], p_rs, partner)

    def y_copy(b):
        return pltpu.make_async_copy(ys, yref(b, whole, 0), ysem)

    def res_copy(b):
        return pltpu.make_async_copy(x_ref.at[pl.ds(pl.multiple_of(b * BLOCK, BLOCK), BLOCK), columns(0, core)], xres, ressem)

    def passes(body, step=32, start=0, size=BLOCK):
        def one(r, _):
            body(pl.ds(pl.multiple_of(start + r * step, step), step))
        lax.fori_loop(0, size // step, one, None)

    def fourth_arrived(b):
        for c in a2_copies(b):
            c.wait_recv()

        @pl.when(b > 0)
        def _():
            p_copy(b, 2).wait_send()
        p_copy(b, 2).start()

    def fourth(b):
        a1_arrived(b)

        @pl.when(b > 0)
        def _():
            for c in (*a2_copies(b), p_copy(b, 0), p_copy(b, 1)):
                c.wait_send()
        for c in (*a2_copies(b, (0,)), p_copy(b, 0), p_copy(b, 1)):
            c.start()

    def fourth_rest(b):
        for c in a2_copies(b, (1,)):
            c.start()

    def third(b):
        res_copy(b).start()
        for c in r2_copies:
            c.wait_recv()

        @pl.when(b > 0)
        def _():
            for c in a1_copies(b):
                c.wait_send()
            y_copy(b).wait()
        res_copy(b).wait()

        def finish(at):
            total = own_s[2, at, :] + r2r[0, at, :].astype(F32) + r2r[1, at, :].astype(F32)
            ys[at, :] = (xres[at, :].astype(F32) + total).astype(BF16)
        passes(finish)

        @pl.when(b < blocks - 1)
        def _():
            signal(r2_free.at[0], right)
            signal(r2_free.at[1], left)

        @pl.when(b < last)
        def _():
            for c in a1_copies(b):
                c.start()
            y_copy(b).start()

        @pl.when(b == last)
        def _():
            pltpu.make_async_copy(ys, last_ref, ysem).start()

    def second(b):
        for c in r1_copies:
            c.wait_recv()

        @pl.when(b > 0)
        def _():
            for c in r2_added:
                c.wait_send()

        def add(at):
            r2s[0, at, :] = (own_s[1, at, :] + r1r[at, :].astype(F32)).astype(BF16)
        passes(add, size=half)

        def add(at):
            r2s[1, at, :] = (own_s[0, at, :] + r1r[at, :].astype(F32)).astype(BF16)
        passes(add, start=half, size=half)

        @pl.when(b < blocks - 1)
        def _():
            signal(r1_free.at[0], right)
            signal(r1_free.at[1], left)
        @pl.when(b > 0)
        def _():
            for n in range(2):
                pl.semaphore_wait(r2_free.at[n], 1)
            for c in r2_alone:
                c.start()
        for c in r2_added:
            c.start()

    def attend(b):
        e = HEAD**-0.5 * LOG2E
        wide = PAIR * BLOCK
        for n in range(heads // PAIR):
            top_s[n] = jnp.full((1, wide), NEG, F32)
            mix_s[n] = jnp.zeros(mix_s.shape[1:], F32)

        def block(j, masked):
            keys = k_s[j]
            values = vt_s[j]
            if masked:
                ok = lax.rem(lax.broadcasted_iota(jnp.int32, (BLOCK, wide), 1), BLOCK) >= lax.broadcasted_iota(jnp.int32, (BLOCK, wide), 0)
            per = 3
            for base in range(0, heads // PAIR, per):
                strips = range(base, min(base + per, heads // PAIR))
                scores = [_dot(keys, q_s[n], 1, 1) for n in strips]
                weights, keeps = [], []
                for n, s in zip(strips, scores):
                    if masked:
                        s = jnp.where(ok, s, HIDDEN)
                    old = top_s[n]
                    top = jnp.maximum(old, s.max(axis=0, keepdims=True))
                    top_s[n] = top
                    weights.append(jnp.exp2((s - top) * e).astype(BF16))
                    keeps.append(jnp.exp2((old - top) * e))
                for n, p, keep in zip(strips, weights, keeps):
                    mix_s[n] = mix_s[n] * keep + _dot(values, p)

        lax.fori_loop(0, b, lambda j, _: block(j, False), None)
        block(b, True)
        for n in range(heads // PAIR):
            out = mix_s[n, :HEAD, :] * (1 / mix_s[n, HEAD : HEAD + 1, :])
            for i in range(PAIR):
                at = (n * PAIR + i) * HEAD
                seen_s[:, at : at + HEAD] = out[:, i * BLOCK : (i + 1) * BLOCK].T.astype(BF16)

    def project_block(b):
        first_tile = b * tiles
        def norm(at):
            total = jnp.zeros((at.size, 1), F32)
            for n in range(0, deep, unit):
                part = xa[at, n : n + unit].astype(F32)
                total += jnp.sum(part * part, axis=1, keepdims=True)
            scale = lax.rsqrt(total / deep + 1e-6)
            for n in range(0, deep, unit):
                part = xa[at, n : n + unit].astype(F32)
                xa[at, n : n + unit] = (part * scale * gains[n : n + unit].astype(F32)[None]).astype(BF16)
        @pl.when(b == 0)
        def _():
            gain_copy.wait()
        for n, c in enumerate(x_copies(b)):
            c.wait()

            @pl.when(b == 0)
            def _():
                if n < 2:
                    start_wq(0, n)
                for c in (kv_copies, (), (table_copy,), ())[n]:
                    c.start()
            passes(norm, 16, n * (BLOCK // PARTS), BLOCK // PARTS)

        qacc[...] = jnp.zeros(qacc.shape, F32)
        kvacc[...] = jnp.zeros(kvacc.shape, F32)

        @pl.when(b == 0)
        def _():
            for c in kv_copies:
                c.wait()
            pl.semaphore_wait(barrier, 3)

        def project(i, _):
            @pl.when((i == SPLIT) & (b == 1))
            def _():
                third(0)
            g = first_tile + i

            @pl.when(i < depth_tiles - 2)
            def _():
                start_wq(b, i + 2)
            for n in range(2):
                @pl.when(i == depth_tiles - 2 + n)
                def _():
                    start_wo(b, n)
            slot = wait_tile(g)
            at = pl.ds(pl.multiple_of(i * unit, unit), unit)
            a = xa[:, at]
            for n in range(0, unit, 512):
                qacc[:, n : n + 512] += _dot(a, wbuf[slot, :, n : n + 512])
            kvacc[...] += _dot(a, wkv[at, :])
        lax.fori_loop(0, depth_tiles, project, None)

        @pl.when(b < blocks - 1)
        def _():
            for c in x_copies(b + 1):
                c.start()

    def rest_of_block(b):
        @pl.when(b == 0)
        def _():
            table_copy.wait()

        first_tile = b * tiles
        at = pl.ds(pl.multiple_of(b * BLOCK, BLOCK), BLOCK)
        cos, sin = table[0, at, :], table[1, at, :]

        def turned(t):
            t = t.astype(BF16).astype(F32)
            return (t * cos + pltpu.roll(t, HEAD // 2, 1) * sin).astype(BF16)
        for n in range(heads):
            i = n % PAIR
            q_s[n // PAIR, i * BLOCK : (i + 1) * BLOCK, :] = turned(qacc[:, n * HEAD : (n + 1) * HEAD])
        k_s[b] = turned(kvacc[:, :HEAD])
        vt_s[b, :HEAD, :] = kvacc[:, HEAD:].T.astype(BF16)
        vt_s[b, HEAD:, :] = jnp.ones((vt_s.shape[1] - HEAD, BLOCK), BF16)
        attend(b)

        for i, (give, j) in enumerate(ORDER):
            if i + 2 < len(ORDER):
                start_wo(b, i + 2)
            else:
                @pl.when(b < blocks - 1)
                def _():
                    start_wq(b + 1, i + 2 - len(ORDER))
            slot = wait_tile(first_tile + depth_tiles + i)
            if give:
                @pl.when(b > 0)
                def _():
                    d_copy(j).wait_send()
                for n in range(0, unit, 512):
                    dsend[j, :, n : n + 512] = _dot(seen_s[...], wbuf[slot, :, n : n + 512]).astype(BF16)

                @pl.when(b > 0)
                def _():
                    pl.semaphore_wait(d_free.at[j], 1)
                d_copy(j).start()
                continue
            d_copy(j).wait_recv()
            if j < 3:
                @pl.when(b > 0)
                def _():
                    for c in (r1_copies, r2_alone[1:], r2_alone[:1])[j]:
                        c.wait_send()
            for n in range(0, unit, 512):
                value = _dot(seen_s[...], wbuf[slot, :, n : n + 512]) + drecv[j, :, n : n + 512].astype(F32)
                if j == 0:
                    r1s[:, n : n + 512] = value.astype(BF16)
                elif j == 1:
                    r2s[1, upper, n : n + 512] = value[:half].astype(BF16)
                    own_s[0, lower, n : n + 512] = value[half:]
                elif j == 2:
                    r2s[0, lower, n : n + 512] = value[half:].astype(BF16)
                    own_s[1, upper, n : n + 512] = value[:half]
                else:
                    own_s[2, :, n : n + 512] = value

            @pl.when(b < blocks - 1)
            def _():
                signal(d_free.at[j], partner)
            if j == 0:
                @pl.when(b > 0)
                def _():
                    for n in range(2):
                        pl.semaphore_wait(r1_free.at[n], 1)
                for c in r1_copies:
                    c.start()
            elif j < 3:
                c = r2_alone[2 - j]

                @pl.when(b == 0)
                def _():
                    c.start()

    for c in (*x_copies(0), gain_copy):
        c.start()
    barrier = pltpu.get_barrier_semaphore()
    for peer in (left, right, partner):
        pl.semaphore_signal(barrier, inc=1, device_id={axis: peer}, device_id_type=MESH)

    def stages(t, which):
        for back, stage in which:
            b = t - back

            end = last - 1 if stage is fourth_arrived else last if stage is fourth else blocks

            @pl.when((b >= 0) & (b < end))
            def _():
                stage(b)

    def step(t, _):
        @pl.when(t < blocks)
        def _():
            project_block(t)

        @pl.when((t > 1) & (t < blocks))
        def _():
            fourth_rest(t - 2)

        @pl.when(t == blocks)
        def _():
            fourth_arrived(last - 1)

        @pl.when(t > 1)
        def _():
            third(t - 1)

        @pl.when(t < blocks)
        def _():
            rest_of_block(t)
        stages(t, ((2, fourth_arrived), (1, fourth)))

        @pl.when(t == last)
        def _():
            fourth_rest(last - 1)
        stages(t, ((0, second),))
    lax.fori_loop(0, blocks + 1, step, None)

    for j in range(RING):
        d_copy(j).wait_send()
    for c in (*r1_copies, *r2_copies, *a2_copies(last - 1), *(p_copy(last - 1, n) for n in range(3))):
        c.wait_send()
    y_copy(last).wait()
    theirs = y_ref.at[pl.ds(0, last * BLOCK), pl.ds(0, RING * unit)]
    pltpu.make_async_copy(theirs, theirs, p_rs).wait()


def _copy_rows(first, count, *refs):
    staged_ref, (y_ref, bufs, ins, outs) = refs[0], refs[-4:]
    size = bufs.shape[1]
    rows = [pl.ds((first + i) * size, size) for i in range(count)]
    loads = [pltpu.make_async_copy(staged_ref.at[at, :], bufs.at[i % COPIES], ins.at[i % COPIES]) for i, at in enumerate(rows)]
    stores = [pltpu.make_async_copy(bufs.at[i % COPIES], y_ref.at[at, :], outs.at[i % COPIES]) for i, at in enumerate(rows)]
    ahead = COPIES // 2
    for i in range(min(ahead, count)):
        loads[i].start()
    for i in range(count):
        loads[i].wait()
        stores[i].start()
        j = i + ahead
        if j < count:
            if j >= COPIES:
                stores[j - COPIES].wait()
            loads[j].start()
    for i in range(max(count - COPIES, 0), count):
        stores[i].wait()


def _rows(staged, first, count, y=None, work=0):
    rows, deep = staged.shape
    size = BLOCK // 8
    given = [staged] if y is None else [staged, y]
    hbm, dma = pl.BlockSpec(memory_space=pl.ANY), pltpu.SemaphoreType.DMA
    return pl.pallas_call(
        functools.partial(_copy_rows, first, count),
        in_specs=[hbm] * len(given),
        out_specs=hbm,
        out_shape=jax.ShapeDtypeStruct(staged.shape, staged.dtype),
        input_output_aliases={} if y is None else {1: 0},
        scratch_shapes=[pltpu.VMEM((COPIES, size, deep), BF16), dma((COPIES,)), dma((COPIES,))],
        compiler_params=pltpu.CompilerParams(vmem_limit_bytes=40 * 2**20),
        cost_estimate=pl.CostEstimate(flops=count * work, bytes_accessed=count * size * deep * 4, transcendentals=0),
    )(*given)


def _place(axis, marks, *refs):
    pieces, (y_ref, buf, ins, outs) = refs[1:-4], refs[-4:]
    unit = buf.shape[2]
    start = y_ref.shape[0] - BLOCK
    me = lax.axis_index(axis)
    chip, core = me // 2, me % 2
    loads, stores = [], []
    for n, (piece, (k, away, row)) in enumerate(zip(pieces, marks)):
        at = pl.ds(pl.multiple_of(((chip + away) % RING) * (2 * unit) + ((core + k) % 2) * unit, unit), unit)
        size = piece.shape[0]
        vmem = buf.at[n, pl.ds(0, size), :]
        loads.append(pltpu.make_async_copy(piece, vmem, ins.at[n]))
        stores.append(pltpu.make_async_copy(vmem, y_ref.at[pl.ds(start + row, size), at], outs.at[n]))
    for c in loads:
        c.start()
    for c, out in zip(loads, stores):
        c.wait()
        out.start()
    for c in stores:
        c.wait()


def _placed(axis, y, marked):
    marks, pieces = zip(*marked)
    hbm, dma = pl.BlockSpec(memory_space=pl.ANY), pltpu.SemaphoreType.DMA
    tall, unit = max(p.shape[0] for p in pieces), pieces[0].shape[1]
    return pl.pallas_call(
        functools.partial(_place, axis, marks),
        out_shape=jax.ShapeDtypeStruct(y.shape, y.dtype),
        in_specs=[hbm] * (1 + len(pieces)),
        out_specs=hbm,
        input_output_aliases={0: 0},
        scratch_shapes=[pltpu.VMEM((len(pieces), tall, unit), BF16), dma((len(pieces),)), dma((len(pieces),))],
        cost_estimate=pl.CostEstimate(flops=4 * WORK, bytes_accessed=4 * sum(p.size for p in pieces), transcendentals=0),
    )(y, *pieces)


def solution(mesh):
    axis = mesh.axis_names[1]
    group = mesh.shape[axis]

    def step(x, gain, wq, wk, wv, wo):
        rows, deep = x.shape
        unit = deep // group
        blocks = rows // BLOCK
        heads = unit // HEAD
        part = HEAD // 2
        angle = np.arange(rows, dtype=np.float32)[:, None] * np.float32(THETA) ** (-np.arange(part, dtype=np.float32) / np.float32(part))
        angle = angle.astype(np.float64)
        cos, sin = (jnp.asarray(f(angle).astype(np.float32)) for f in (np.cos, np.sin))
        table = jnp.stack([jnp.concatenate([cos, cos], 1), jnp.concatenate([-sin, sin], 1)])
        vmem, hbm = pl.BlockSpec(memory_space=pltpu.VMEM), pl.BlockSpec(memory_space=pl.ANY)
        dma, regular = pltpu.SemaphoreType.DMA, pltpu.SemaphoreType.REGULAR
        strips = heads // PAIR
        staged, mine = pl.pallas_call(
            functools.partial(_layer, axis),
            out_shape=[jax.ShapeDtypeStruct((rows, deep), BF16), jax.ShapeDtypeStruct((BLOCK, unit), BF16)],
            in_specs=[hbm] * 7,
            out_specs=[hbm, hbm],
            scratch_shapes=[
                pltpu.VMEM((BLOCK, deep), BF16),
                pltpu.VMEM((2, rows, HEAD), F32),
                pltpu.VMEM((deep,), BF16),
                pltpu.VMEM((BUFFERS, unit, unit), BF16),
                pltpu.VMEM((deep, 2 * HEAD), BF16),
                pltpu.VMEM((BLOCK, unit), F32),
                pltpu.VMEM((BLOCK, 2 * HEAD), F32),
                pltpu.VMEM((strips, PAIR * BLOCK, HEAD), BF16),
                pltpu.VMEM((blocks, BLOCK, HEAD), BF16),
                pltpu.VMEM((blocks, HEAD + 16, BLOCK), BF16),
                pltpu.VMEM((strips, 1, PAIR * BLOCK), F32),
                pltpu.VMEM((strips, HEAD + 16, PAIR * BLOCK), F32),
                pltpu.VMEM((BLOCK, unit), BF16),
                pltpu.VMEM((RING - 1, BLOCK, unit), F32),
                pltpu.VMEM((RING, BLOCK, unit), BF16),
                pltpu.VMEM((RING, BLOCK, unit), BF16),
                pltpu.VMEM((BLOCK, unit), BF16),
                pltpu.VMEM((BLOCK, unit), BF16),
                pltpu.VMEM((2, BLOCK, unit), BF16),
                pltpu.VMEM((2, BLOCK, unit), BF16),
                pltpu.VMEM((BLOCK, unit), BF16),
                pltpu.VMEM((BLOCK, unit), BF16),
                dma((BUFFERS,)), dma((PARTS,)), dma, dma, dma((2,)), dma, dma,
                dma((RING,)), dma((RING,)), regular((RING,)),
                dma((2,)), dma((2,)), regular((2,)),
                dma((4,)), dma((4,)), regular((2,)),
                dma((3,)), dma((2, 2)),
                dma((4,)), dma((2, 4)),
                dma((3,)), dma,
            ],
            compiler_params=pltpu.CompilerParams(collective_id=0, has_side_effects=True, vmem_limit_bytes=VMEM),
        )(x, gain, table, wq, wk, wv, wo)

        def hop(value, chips, cores):
            return lax.ppermute(value, axis, [(t, (t + 2 * chips) % group // 2 * 2 + (t + cores) % 2) for t in range(group)])

        count = 8 * (rows // BLOCK - 1)
        early = count * FIRST // 28
        half = BLOCK // 2
        from_left, from_right, beside = hop(mine, 1, 0), hop(mine, -1, 0), hop(mine, 0, 1)
        y = _rows(staged, 0, early, work=WORK)
        y, from_left, from_right = lax.optimization_barrier((y, from_left, from_right))
        upper, lower = hop(from_left[:half], 1, 0), hop(from_right[half:], -1, 0)
        marked = [((0, 0, 0), mine), ((1, 0, 0), beside), ((0, RING - 1, 0), from_left), ((0, 1, 0), from_right),
                  ((1, RING - 1, 0), hop(from_left, 0, 1)), ((1, 1, 0), hop(from_right, 0, 1))]
        y = _rows(staged, early, count - early, y, work=WORK)
        y, upper, lower = lax.optimization_barrier((y, upper, lower))
        late = [((0, 2, 0), upper), ((0, 2, half), lower), ((1, 2, 0), hop(upper, 0, 1)), ((1, 2, half), hop(lower, 0, 1))]
        return _placed(axis, _placed(axis, y, marked), late)

    tokens, columns = P(mesh.axis_names[0], None), P(None, axis)
    return jax.shard_map(
        step,
        mesh=mesh,
        in_specs=(tokens, P(None), columns, columns, columns, P(axis, None)),
        out_specs=tokens,
        check_vma=False,
    )
```
